256 devices in a mesh: row: 8 (over x, y_lo), blk: 32 (over y_hi, z, core).
Axes of the slice: x: 4, y: 4 (y_hi: 2, y_lo: 2; y = y_hi * 2 + y_lo), z: 8, core: 2. Of those that a mesh axis runs over, the one named last changes fastest.
Arguments:
- elastic_kernel: bfloat16 [32, 1024, 8, 4096], P('blk', None, 'row'), may hold values from -0.046875 to 0.046875
- slip_deficit: float32 [32, 8, 128, 512], P('blk', 'row'), may hold values from -6 to 6
- state_variable: float32 [32, 8, 128, 512], P('blk', 'row'), may hold values from 0.2 to 5
- step_size: float32 [512], replicated, may hold values from 0.02 to 0.1
- load_stress: float32 [32, 8, 128], P('blk', 'row'), may hold values from -6 to 6
- normal_stress: float32 [32, 8, 128], P('blk', 'row'), may hold values from 0.5 to 2
- rate_table: float32 [16], replicated, may hold values from 0.3 to 1
- evolve_table: float32 [16], replicated, may hold values from 0.3 to 1.5
- patch_region: int32 [32, 8, 128], P('blk', 'row'), may hold values from 0 to 15
- creep_flag: int32 [32, 8, 128], P('blk', 'row'), may hold values 0 or 1
Outputs:
- velocity: float32 [32, 8, 128, 512], P('blk', 'row')
- deficit_out: float32 [32, 8, 128, 512], P('blk', 'row')
- state_out: float32 [32, 8, 128, 512], P('blk', 'row')
- step_next: float32 [512], replicated
The draws below stay inside these ranges and needn't reach their ends.
All inputs are finite; a program needn't handle non-finite values. Where the reference program divides by a largest or mean magnitude, that divisor is 1e-20 or more. No bound on the sum of `creep_flag` on one device may be relied on, other than what follows from the above.
Results may differ from the reference program's by a relative error of at most 0.0035.
Values may be sent and summed in bfloat16 or wider, within the bound.
A program may use at most 64 MiB of HBM per device.

```python
import math
import jax
import jax.numpy as jnp
from jax import lax

ELEM_DEV = 128
MEMBERS = 512
REGIONS = 16
NEWTON = 3
STEPS = 2
ROW_GROUPS = 8
COL_BLOCKS = 32
ELEMENTS = 32768


def touch_ends(array, own_key, least, high):
    longest = array.shape.index(max(array.shape))
    spots = []
    for shift in (0, 1):
        where = [jax.random.randint(jax.random.fold_in(own_key, axis), (), 0, length) for axis, length in enumerate(array.shape)]
        where[longest] = (where[longest] + shift) % array.shape[longest]
        spots.append(tuple(where))
    return array.at[spots[0]].set(least).at[spots[1]].set(high)


def strengthened(array, key, source, target, blocks, factor):
    def block_of(dim):
        return (jnp.arange(array.shape[dim]) // (array.shape[dim] // blocks)).reshape((-1,) + (1,) * (array.ndim - 1 - dim))

    near = jax.random.permutation(key, blocks)[block_of(target)]
    far = (block_of(target) + blocks // 2) % blocks
    return jnp.where((block_of(source) == near) | (block_of(source) == far), factor * array, array)


def steps_of(own_key, extent, shards, least, top_value):
    def one(position, blocks):
        steps = jax.random.uniform(jax.random.fold_in(jax.random.fold_in(own_key, 6), position), (blocks,), jnp.float32, least / len(shards), top_value / len(shards))
        return jnp.repeat(jnp.exp(steps), extent[position] // blocks).reshape((-1,) + (1,) * (len(extent) - position - 1))

    gain = one(*shards[0])
    for cut in shards[1:]:
        gain = gain * one(*cut)
    return gain


def gaussian(rng, shape, width, reach, pieces=(), kind=jnp.bfloat16):
    values = jax.random.normal(rng, shape, jnp.float32) * width
    if len(pieces) > 0:
        values = steps_of(rng, shape, pieces, -0.22, 0.18) * values
    return jnp.clip(values, min=-reach, max=reach).astype(kind)


def bell_draw_with(rng, shape, spread, reach, shards, heavy, held_as=jnp.bfloat16):
    values = spread * jax.random.normal(rng, shape, jnp.float32)
    if shards:
        values = values * steps_of(rng, shape, shards, -0.22, 0.18)
    return jnp.clip(strengthened(values, jax.random.fold_in(rng, 3), *heavy), -reach, reach).astype(held_as)


def setup_inputs(seed: int = 0) -> dict:
    splits = jax.random.split(jax.random.key(seed), 11)
    elastic_kernel = bell_draw_with(splits[0], (COL_BLOCKS, ROW_GROUPS * ELEM_DEV, ROW_GROUPS, COL_BLOCKS * ELEM_DEV), ELEMENTS ** -0.5, 0.046875, ((0, 32), (2, 8)), (2, 1, 8, 2.0))
    slip_deficit = gaussian(splits[1], (COL_BLOCKS, ROW_GROUPS, ELEM_DEV, MEMBERS), 1.0, 6.0, ((0, 32), (1, 8)), jnp.float32)
    state_variable = jnp.clip(jnp.exp(math.log(5.0) - 3.218876 * jax.random.uniform(splits[2], (COL_BLOCKS, ROW_GROUPS, ELEM_DEV, MEMBERS), jnp.float32) ** steps_of(splits[2], (COL_BLOCKS, ROW_GROUPS, ELEM_DEV, MEMBERS), ((0, 32), (1, 8)), -0.2, 0.2)), 0.2, 5.0)
    step_size = jnp.clip(jnp.exp(jax.random.uniform(splits[3], (MEMBERS,), jnp.float32, math.log(0.02), math.log(0.1))), 0.02, 0.1)
    load_stress = gaussian(splits[4], (COL_BLOCKS, ROW_GROUPS, ELEM_DEV), 1.0, 6.0, ((0, 32), (1, 8)), jnp.float32)
    normal_stress = jnp.clip(jnp.exp(math.log(2.0) - 1.3862944 * jax.random.uniform(splits[5], (COL_BLOCKS, ROW_GROUPS, ELEM_DEV), jnp.float32) ** steps_of(splits[5], (COL_BLOCKS, ROW_GROUPS, ELEM_DEV), ((0, 32), (1, 8)), -0.2, 0.2)), 0.5, 2.0)
    rate_table = jnp.clip(jnp.exp(jax.random.uniform(splits[6], (REGIONS,), jnp.float32, math.log(0.3), math.log(1.0))), 0.3, 1.0)
    evolve_table = jnp.clip(jnp.exp(jax.random.uniform(splits[7], (REGIONS,), jnp.float32, math.log(0.3), math.log(1.5))), 0.3, 1.5)
    patch_region = touch_ends(jax.random.randint(splits[8], (COL_BLOCKS, ROW_GROUPS, ELEM_DEV), 0, REGIONS), jax.random.fold_in(splits[8], 1), 0, REGIONS - 1).astype(jnp.int32)
    creep_flag = touch_ends((jax.random.randint(splits[9], (COL_BLOCKS, ROW_GROUPS, ELEM_DEV), 0, 4) < 1).astype(jnp.int32), jax.random.fold_in(splits[9], 1), 0, 1)
    return {"elastic_kernel": elastic_kernel, "slip_deficit": slip_deficit, "state_variable": state_variable, "step_size": step_size, "load_stress": load_stress, "normal_stress": normal_stress, "rate_table": rate_table, "evolve_table": evolve_table, "patch_region": patch_region, "creep_flag": creep_flag}


DAMPING = 0.5
PLATE_RATE = 1.0
STEP_CAP = 0.5

def inverse_sinh(value):
    magnitude = jnp.abs(value)
    result = jnp.log(magnitude + jnp.sqrt(magnitude * magnitude + 1.0))
    return jnp.where(value < 0.0, -result, result)

def tractions(elastic_kernel, deficit):
    slip = deficit.astype(jnp.bfloat16)
    sources = jnp.transpose(slip, (1, 0, 2, 3)).reshape(-1, slip.shape[3])

    def one_block(kernel_block):
        flat = kernel_block.reshape(kernel_block.shape[0], -1)
        return jnp.dot(flat, sources, preferred_element_type=jnp.float32)
    result = lax.map(one_block, elastic_kernel)
    return result.reshape(slip.shape)

def solve_rate(stress, pressure, rate_coef, state_coef, state, creeping):
    factor = 0.5 * jnp.exp(state_coef * jnp.log(state) / rate_coef)
    strength = pressure * rate_coef
    speed = stress / (strength * factor + DAMPING)
    for repeat in range(NEWTON):
        scaled = factor * speed
        mismatch = strength * inverse_sinh(scaled) + DAMPING * speed - stress
        gradient = strength * factor / jnp.sqrt(1.0 + scaled * scaled) + DAMPING
        speed = speed - mismatch / gradient
    return jnp.where(creeping, jnp.float32(PLATE_RATE), speed)

def reference(elastic_kernel, slip_deficit, state_variable, step_size, load_stress, normal_stress, rate_table, evolve_table, patch_region, creep_flag):
    levels = jnp.arange(rate_table.shape[0], dtype=jnp.int32)
    onehot = (patch_region[..., None] == levels).astype(jnp.float32)
    rate_coef = lax.optimization_barrier(jnp.sum(onehot * rate_table, axis=-1))[..., None]
    state_coef = lax.optimization_barrier(jnp.sum(onehot * evolve_table, axis=-1))[..., None]
    pressure = normal_stress[..., None]
    loading = load_stress[..., None]
    creeping = (creep_flag == 1)[..., None]
    deficit = slip_deficit
    state = state_variable
    step_now = step_size
    velocity = jnp.zeros_like(deficit)
    for repeat in range(STEPS):
        stress = loading + tractions(elastic_kernel, deficit)
        velocity = solve_rate(stress, pressure, rate_coef, state_coef, state, creeping)
        largest = lax.optimization_barrier(jnp.max(jnp.abs(velocity), axis=(0, 1, 2)))
        state = state * jnp.exp(step_now * (1.0 / state - jnp.abs(velocity)))
        deficit = deficit + step_now * (velocity - PLATE_RATE)
        step_now = STEP_CAP / (1.0 + largest)
    return (velocity, deficit, state, step_now)
```

```python
import functools

import jax
import jax.numpy as jnp
from jax import lax
from jax.experimental import pallas as pl
from jax.experimental.pallas import tpu as pltpu
from jax.sharding import Mesh
from jax.sharding import PartitionSpec as P

NEWTON = 3
DAMPING = 0.5
PLATE_RATE = 1.0
STEP_CAP = 0.5

AXES = ("row_0", "row_1", "blk_0", "blk_1", "blk_2")
BLK = ("blk_0", "blk_1", "blk_2")
ROW = ("row_0", "row_1")
MESH = pl.DeviceIdType.MESH

CHUNKS = 2
E = 128
ORDER = (0, 7, 1, 6, 2, 5, 3, 4)
GROUPS = ((0, 4), (4, 12), (12, 20), (20, 32))


def slot(plane, offset, core):
    return ORDER.index(offset) * 4 + plane * 2 + core


def kernel_body(
    k_hbm,
    deficit_hbm,
    state_hbm,
    step_hbm,
    load_hbm,
    normal_hbm,
    rate_hbm,
    evolve_hbm,
    region_hbm,
    creep_hbm,
    v_out,
    d_out,
    s_out,
    step_out,
    kv,
    gathered,
    acc,
    own_sum,
    xsend,
    xrecv,
    ysend,
    yrecv,
    deficit,
    state,
    factor,
    vel,
    step_in,
    load_in,
    normal_in,
    rate_in,
    evolve_in,
    region_in,
    creep_in,
    cols,
    top,
    mid,
    top_recv,
    mid_recv,
    step_fin,
    k_sem,
    in_sem,
    out_sem,
    send_sem,
    recv_sem,
    max_send,
    max_recv,
):
    members = deficit.shape[1]
    width = members // CHUNKS
    x = lax.axis_index("row_0")
    yl = lax.axis_index("row_1")
    yh = lax.axis_index("blk_0")
    z = lax.axis_index("blk_1")
    core = lax.axis_index("blk_2")

    z_up = {"blk_1": lax.rem(z + 1, 8)}
    z_down = {"blk_1": lax.rem(z + 7, 8)}
    y_far = {"blk_0": 1 - yh}
    sibling = {"blk_2": 1 - core}
    y_near = {"row_1": 1 - yl}
    x_peer = {k: {"row_0": lax.rem(x + k, 4)} for k in (1, 2, 3)}
    plane_peers = [
        {"row_0": lax.rem(x + dx, 4), "row_1": (yl + dl) % 2, "blk_0": (yh + dh) % 2}
        for dx in range(4)
        for dl in range(2)
        for dh in range(2)
        if dx or dl or dh
    ]
    line_peers = [
        {"blk_1": lax.rem(z + dz, 8), "blk_2": (core + dc) % 2}
        for dz in range(8)
        for dc in range(2)
        if dz or dc
    ]

    loads = []
    for i, (src, dst) in enumerate(
        (
            (deficit_hbm, deficit),
            (step_hbm, step_in),
            (load_hbm, load_in),
            (normal_hbm, normal_in),
            (rate_hbm, rate_in),
            (evolve_hbm, evolve_in),
            (region_hbm, region_in),
            (creep_hbm, creep_in),
            (state_hbm, state),
        )
    ):
        copy = pltpu.make_async_copy(src, dst, in_sem.at[i])
        copy.start()
        loads.append(copy)

    barrier = pltpu.get_barrier_semaphore()
    for peer in plane_peers + line_peers:
        pl.semaphore_signal(barrier, inc=1, device_id=peer, device_id_type=MESH)

    for group, (low, high) in enumerate(GROUPS):
        for at in range(low, high):
            offset, plane, cr = ORDER[at // 4], (at // 2) % 2, at % 2
            block = (((yh + plane) % 2) * 8 + lax.rem(z + offset, 8)) * 2 + (core + cr) % 2
            pltpu.make_async_copy(
                k_hbm.at[:, pl.ds(pl.multiple_of(block * E, E), E)],
                kv.at[:, pl.ds(at * E, E)],
                k_sem.at[group],
            ).start()

    sent = []
    flight = {}

    def send(phase, key, src, dst, number, device):
        copy = pltpu.make_async_remote_copy(
            src_ref=src,
            dst_ref=dst,
            send_sem=send_sem.at[phase, number],
            recv_sem=recv_sem.at[phase, number],
            device_id=device,
            device_id_type=MESH,
        )
        copy.start()
        sent.append(copy)
        flight[(phase, key)] = copy

    def arrived(phase, *keys):
        for key in keys:
            flight[(phase, key)].wait_recv()

    def rows_of(phase, at, half=None):
        if half is None:
            return gathered.at[phase, pl.ds(at * E, E)]
        return gathered.at[phase, pl.ds(at * E + half * (E // 2), E // 2)]

    numbers = {}

    def number_of(key):
        return numbers.setdefault(key, len(numbers))

    def move(phase, plane, offset, to_plane, to_offset, device, half=None):
        key = (to_plane, to_offset, half)
        send(
            phase,
            key,
            rows_of(phase, slot(plane, offset, 0), half),
            rows_of(phase, slot(to_plane, to_offset, 0), half),
            number_of(key),
            device,
        )

    def share(phase, plane, offset):
        key = ("core", plane, offset)
        send(
            phase,
            key,
            rows_of(phase, slot(plane, offset, 0)),
            rows_of(phase, slot(plane, offset, 1)),
            number_of(key),
            sibling,
        )

    def shared(phase, *blocks):
        arrived(phase, *(("core", plane, offset) for plane, offset in blocks))

    def round_0(phase):
        move(phase, 0, 0, 0, 7, z_up)
        move(phase, 0, 0, 0, 1, z_down)
        move(phase, 0, 0, 1, 0, y_far)
        share(phase, 0, 0)

    def round_1(phase):
        arrived(phase, (0, 7, None))
        move(phase, 0, 7, 0, 6, z_up)
        arrived(phase, (0, 1, None))
        move(phase, 0, 1, 0, 2, z_down)
        arrived(phase, (1, 0, None))
        move(phase, 1, 0, 1, 7, z_up)
        move(phase, 1, 0, 1, 1, z_down)
        share(phase, 1, 0)
        share(phase, 0, 7)
        share(phase, 0, 1)

    def round_2(phase):
        arrived(phase, (0, 6, None))
        move(phase, 0, 6, 0, 5, z_up)
        move(phase, 0, 6, 1, 6, y_far, 1)
        arrived(phase, (0, 2, None))
        move(phase, 0, 2, 0, 3, z_down)
        move(phase, 0, 2, 1, 2, y_far, 1)
        arrived(phase, (1, 7, None))
        move(phase, 1, 7, 1, 6, z_up, 0)
        arrived(phase, (1, 1, None))
        move(phase, 1, 1, 1, 2, z_down, 0)
        share(phase, 0, 6)
        share(phase, 0, 2)
        share(phase, 1, 7)
        share(phase, 1, 1)

    def round_3(phase):
        arrived(phase, (0, 5, None))
        move(phase, 0, 5, 0, 4, z_up, 0)
        move(phase, 0, 5, 1, 5, y_far)
        arrived(phase, (0, 3, None))
        move(phase, 0, 3, 0, 4, z_down, 1)
        move(phase, 0, 3, 1, 3, y_far)
        share(phase, 0, 5)
        share(phase, 0, 3)
        arrived(phase, (1, 6, 0), (1, 6, 1))
        share(phase, 1, 6)
        arrived(phase, (1, 2, 0), (1, 2, 1))
        share(phase, 1, 2)

    def round_4(phase):
        arrived(phase, (0, 4, 0), (0, 4, 1))
        move(phase, 0, 4, 1, 4, y_far)
        share(phase, 0, 4)
        arrived(phase, (1, 5, None))
        share(phase, 1, 5)
        arrived(phase, (1, 3, None))
        share(phase, 1, 3)
        arrived(phase, (1, 4, None))
        share(phase, 1, 4)

    def product(phase, group, rows):
        low, high = GROUPS[group]
        return jnp.dot(
            kv[rows, low * E : high * E],
            gathered[phase, low * E : high * E, :],
            preferred_element_type=jnp.float32,
        )

    def multiply(phase, chunk, group):
        if phase == 0:
            low, high = GROUPS[group]
            part = kv.at[:, pl.ds(low * E, (high - low) * E)]
            pltpu.make_async_copy(part, part, k_sem.at[group]).wait()

        def tile(i, carry):
            rows = pl.ds(pl.multiple_of(i * 256, 256), 256)
            value = product(phase, group, rows)
            if group == 0:
                acc[chunk, rows] = value
            else:
                acc[chunk, rows] += value
            return carry

        lax.fori_loop(0, 4, tile, 0)

    def multiply_last(phase, chunk):
        group = len(GROUPS) - 1
        if phase == 0:
            low, high = GROUPS[group]
            part = kv.at[:, pl.ds(low * E, (high - low) * E)]
            pltpu.make_async_copy(part, part, k_sem.at[group]).wait()
        for dx in (2, 1, 3, 0):
            rows = pl.ds(pl.multiple_of(lax.rem(x + dx, 4) * 256, 256), 256)
            value = acc[chunk, rows] + product(phase, group, rows)
            if dx:
                xsend[phase, dx - 1] = value.astype(jnp.bfloat16)
                send(
                    phase,
                    ("x", dx),
                    xsend.at[phase, dx - 1],
                    xrecv.at[phase, dx - 1],
                    number_of(("x", dx)),
                    x_peer[dx],
                )
            else:
                own_sum[chunk] = value

    def reduce_x(phase, chunk):
        arrived(phase, ("x", 1), ("x", 2), ("x", 3))
        other = pl.multiple_of((1 - yl) * E, E)
        mine = pl.multiple_of(yl * E, E)

        def tile(i, carry):
            for base, target in ((other, 0), (mine, 1)):
                rows = pl.ds(pl.multiple_of(base + i * 32, 32), 32)
                total = own_sum[chunk, rows]
                for k in range(3):
                    total = total + xrecv[phase, k, rows].astype(jnp.float32)
                if target == 0:
                    ysend[phase, pl.ds(pl.multiple_of(i * 32, 32), 32)] = total.astype(jnp.bfloat16)
                else:
                    own_sum[chunk, rows] = total
            return carry

        lax.fori_loop(0, 4, tile, 0)
        send(phase, "y", ysend.at[phase], yrecv.at[phase], number_of("y"), y_near)

    def set_factor(chunk):
        lanes = slice(chunk * width, (chunk + 1) * width)

        def tile(i, carry):
            rows = pl.ds(pl.multiple_of(i * 32, 32), 32)
            rate = cols[rows, 2:3]
            evolve = cols[rows, 3:4]
            factor[chunk, rows] = 0.5 * jnp.exp(evolve * jnp.log(state[rows, lanes]) / rate)
            return carry

        lax.fori_loop(0, 4, tile, 0)

    def solve(phase, chunk, step):
        lanes = slice(chunk * width, (chunk + 1) * width)
        mine = pl.multiple_of(yl * E, E)
        arrived(phase, "y")
        step_now = step_in[:, lanes]

        def tile(i, carry):
            rows = pl.ds(pl.multiple_of(i * 32, 32), 32)
            from_rows = pl.ds(pl.multiple_of(mine + i * 32, 32), 32)
            loading = cols[rows, 0:1]
            strength = cols[rows, 1:2] * cols[rows, 2:3]
            creeping = cols[rows, 4:5]
            stress = loading + (own_sum[chunk, from_rows] + yrecv[phase, rows].astype(jnp.float32))
            scale = factor[chunk, rows]
            slope = strength * scale
            speed = stress / (slope + DAMPING)
            for _ in range(NEWTON):
                scaled = scale * speed
                magnitude = jnp.abs(scaled)
                root = jnp.sqrt(magnitude * magnitude + 1.0)
                arc = jnp.log(magnitude + root)
                arc = jnp.where(scaled < 0.0, -arc, arc)
                mismatch = strength * arc + DAMPING * speed - stress
                gradient = slope / root + DAMPING
                speed = speed - mismatch / gradient
            speed = jnp.where(creeping > 0.5, jnp.float32(PLATE_RATE), speed)
            size = jnp.abs(speed)
            if step == 0:
                old = state[rows, lanes]
                state[rows, lanes] = old * jnp.exp(step_now * (1.0 / old - size))
                moved = deficit[rows, lanes] + step_now * (speed - PLATE_RATE)
                deficit[rows, lanes] = moved
                gathered[phase + CHUNKS, pl.ds(pl.multiple_of(i * 32, 32), 32)] = moved.astype(jnp.bfloat16)
            else:
                vel[rows, lanes] = speed
            return jnp.maximum(carry, jnp.max(size.reshape(4, 8, width), axis=0))

        largest = lax.fori_loop(0, 4, tile, jnp.zeros((8, width), jnp.float32))
        top[step, :, lanes] = jnp.max(largest, axis=0, keepdims=True)

    max_copies = {}

    def max_send_all(step, stage):
        peers = plane_peers if stage == 0 else line_peers
        source = top if stage == 0 else mid
        target = top_recv if stage == 0 else mid_recv
        copies = []
        for k, peer in enumerate(peers):
            copy = pltpu.make_async_remote_copy(
                src_ref=source.at[step],
                dst_ref=target.at[step, k],
                send_sem=max_send.at[step, stage, k],
                recv_sem=max_recv.at[step, stage, k],
                device_id=peer,
                device_id_type=MESH,
            )
            copy.start()
            copies.append(copy)
            sent.append(copy)
        max_copies[(step, stage)] = copies

    def max_take(step, stage):
        for copy in max_copies[(step, stage)]:
            copy.wait_recv()
        source = top if stage == 0 else mid
        target = top_recv if stage == 0 else mid_recv
        return jnp.maximum(source[step], jnp.max(target[step], axis=0))

    loads[0].wait()
    for chunk in range(CHUNKS):
        gathered[chunk, 0:E] = deficit[:, chunk * width : (chunk + 1) * width].astype(jnp.bfloat16)
    for copy in loads[1:]:
        copy.wait()
    region = region_in[...]
    rate_row = jnp.zeros((1, E), jnp.float32)
    evolve_row = jnp.zeros((1, E), jnp.float32)
    for level in range(rate_in.shape[1]):
        chosen = region == level
        rate_row = jnp.where(chosen, rate_in[:, level : level + 1], rate_row)
        evolve_row = jnp.where(chosen, evolve_in[:, level : level + 1], evolve_row)
    creep_row = jnp.where(creep_in[...] == 1, 1.0, 0.0).astype(jnp.float32)
    picked = lax.broadcasted_iota(jnp.int32, (E, E), 0)
    stacked = jnp.zeros((E, E), jnp.float32)
    for k, row in enumerate((load_in[...], normal_in[...], rate_row, evolve_row, creep_row)):
        stacked = jnp.where(picked == k, jnp.broadcast_to(row, (E, E)), stacked)
    cols[...] = stacked.T

    pl.semaphore_wait(barrier, len(plane_peers) + len(line_peers))

    first = list(range(CHUNKS))
    for chunk in first:
        round_0(chunk)
    for chunk in first:
        set_factor(chunk)

    for step in range(2):
        phases = [step * CHUNKS + chunk for chunk in range(CHUNKS)]
        for chunk, phase in enumerate(phases):
            round_1(phase)
        for chunk, phase in enumerate(phases):
            round_2(phase)
            shared(phase, (0, 0), (1, 0))
            multiply(phase, chunk, 0)
        for chunk, phase in enumerate(phases):
            round_3(phase)
            shared(phase, (0, 7), (0, 1), (1, 7), (1, 1))
            multiply(phase, chunk, 1)
            if step == 1 and chunk == 0:
                mid[0] = max_take(0, 0)
                max_send_all(0, 1)
        for chunk, phase in enumerate(phases):
            round_4(phase)
            shared(phase, (0, 6), (0, 2), (1, 6), (1, 2))
            multiply(phase, chunk, 2)
            shared(phase, (0, 5), (0, 3), (0, 4), (1, 5), (1, 3), (1, 4))
            multiply_last(phase, chunk)
        for chunk, phase in enumerate(phases):
            reduce_x(phase, chunk)
        for chunk, phase in enumerate(phases):
            solve(phase, chunk, step)
            if step == 0:
                round_0(phase + CHUNKS)
        max_send_all(step, 0)
        if step == 0:
            for chunk in range(CHUNKS):
                set_factor(chunk)

    outs = []

    def put(src, dst, i):
        copy = pltpu.make_async_copy(src, dst, out_sem.at[i])
        copy.start()
        outs.append(copy)

    put(vel, v_out, 0)
    step_last = STEP_CAP / (1.0 + max_take(0, 1))

    def finish(i, carry):
        rows = pl.ds(pl.multiple_of(i * 16, 16), 16)
        speed = vel[rows]
        old = state[rows]
        state[rows] = old * jnp.exp(step_last * (1.0 / old - jnp.abs(speed)))
        deficit[rows] = deficit[rows] + step_last * (speed - PLATE_RATE)
        return carry

    lax.fori_loop(0, 8, finish, 0)
    put(deficit, d_out, 1)
    put(state, s_out, 2)
    mid[1] = max_take(1, 0)
    max_send_all(1, 1)
    step_fin[...] = STEP_CAP / (1.0 + max_take(1, 1))
    put(step_fin, step_out, 3)
    for copy in outs:
        copy.wait()
    for copy in sent:
        copy.wait_send()


def body(
    elastic_kernel,
    slip_deficit,
    state_variable,
    step_size,
    load_stress,
    normal_stress,
    rate_table,
    evolve_table,
    patch_region,
    creep_flag,
):
    members = slip_deficit.shape[3]
    width = members // CHUNKS
    phases = 2 * CHUNKS
    regions = rate_table.shape[0]
    f32, bf16, i32 = jnp.float32, jnp.bfloat16, jnp.int32
    anywhere = pl.BlockSpec(memory_space=pl.ANY)
    whole = jax.ShapeDtypeStruct((E, members), f32)
    scratch = [
        pltpu.VMEM((1024, 4096), bf16),
        pltpu.VMEM((phases, 4096, width), bf16),
        pltpu.VMEM((CHUNKS, 1024, width), f32),
        pltpu.VMEM((CHUNKS, 256, width), f32),
        pltpu.VMEM((phases, 3, 256, width), bf16),
        pltpu.VMEM((phases, 3, 256, width), bf16),
        pltpu.VMEM((phases, E, width), bf16),
        pltpu.VMEM((phases, E, width), bf16),
        pltpu.VMEM((E, members), f32),
        pltpu.VMEM((E, members), f32),
        pltpu.VMEM((CHUNKS, E, width), f32),
        pltpu.VMEM((E, members), f32),
        pltpu.VMEM((1, members), f32),
        pltpu.VMEM((1, E), f32),
        pltpu.VMEM((1, E), f32),
        pltpu.VMEM((1, regions), f32),
        pltpu.VMEM((1, regions), f32),
        pltpu.VMEM((1, E), i32),
        pltpu.VMEM((1, E), i32),
        pltpu.VMEM((E, E), f32),
        pltpu.VMEM((2, 1, members), f32),
        pltpu.VMEM((2, 1, members), f32),
        pltpu.VMEM((2, 15, 1, members), f32),
        pltpu.VMEM((2, 15, 1, members), f32),
        pltpu.VMEM((1, members), f32),
        pltpu.SemaphoreType.DMA((len(GROUPS),)),
        pltpu.SemaphoreType.DMA((9,)),
        pltpu.SemaphoreType.DMA((4,)),
        pltpu.SemaphoreType.DMA((phases, 40)),
        pltpu.SemaphoreType.DMA((phases, 40)),
        pltpu.SemaphoreType.DMA((2, 2, 15)),
        pltpu.SemaphoreType.DMA((2, 2, 15)),
    ]
    velocity, deficit, state, step_next = pl.pallas_call(
        kernel_body,
        out_shape=(whole, whole, whole, jax.ShapeDtypeStruct((1, members), f32)),
        in_specs=[anywhere] * 10,
        out_specs=(anywhere,) * 4,
        scratch_shapes=scratch,
        compiler_params=pltpu.CompilerParams(
            collective_id=0, has_side_effects=True, vmem_limit_bytes=60 * 1024 * 1024
        ),
        name="fault_steps",
    )(
        elastic_kernel.reshape(1024, 4096),
        slip_deficit.reshape(E, members),
        state_variable.reshape(E, members),
        step_size.reshape(1, members),
        load_stress.reshape(1, E),
        normal_stress.reshape(1, E),
        rate_table.reshape(1, regions),
        evolve_table.reshape(1, regions),
        patch_region.reshape(1, E),
        creep_flag.reshape(1, E),
    )
    shape = slip_deficit.shape
    return velocity.reshape(shape), deficit.reshape(shape), state.reshape(shape), step_next.reshape(members)


def solution(mesh):
    torus = Mesh(mesh.devices.reshape(4, 2, 2, 8, 2), AXES)
    in_specs = (
        P(BLK, None, ROW, None),
        P(BLK, ROW, None, None),
        P(BLK, ROW, None, None),
        P(),
        P(BLK, ROW, None),
        P(BLK, ROW, None),
        P(),
        P(),
        P(BLK, ROW, None),
        P(BLK, ROW, None),
    )
    out_specs = (P(BLK, ROW, None, None), P(BLK, ROW, None, None), P(BLK, ROW, None, None), P())
    return jax.shard_map(body, mesh=torus, in_specs=in_specs, out_specs=out_specs, check_vma=False)
```

```python
import functools
import itertools

import jax
import jax.numpy as jnp
from jax import lax
from jax.experimental import pallas as pl
from jax.experimental.pallas import tpu as pltpu
from jax.sharding import Mesh
from jax.sharding import PartitionSpec as P

NEWTON = 3
DAMPING = 0.5
PLATE_RATE = 1.0
STEP_CAP = 0.5

AXES = ("row_0", "row_1", "blk_0", "blk_1", "blk_2")
BLK = ("blk_0", "blk_1", "blk_2")
ROW = ("row_0", "row_1")
MESH = pl.DeviceIdType.MESH

CHUNKS = 2
E = 128
TILE = 64
ROW_OFFSETS = ((2, 1), (2, 0), (1, 1), (3, 1), (1, 0), (3, 0), (0, 1))
OFFSETS = ((0,), (7, 1), (6, 2), (5, 3, 4))
GROUPS = ((0, 4), (4, 12), (12, 20), (20, 32))


LIMIT = 62


def slot(plane, offset, core):
    group = next(g for g, offsets in enumerate(OFFSETS) if offset in offsets)
    offsets = OFFSETS[group]
    return GROUPS[group][0] + (core * 2 + plane) * len(offsets) + offsets.index(offset)


def kernel_body(
    k_hbm,
    deficit_hbm,
    state_hbm,
    step_hbm,
    load_hbm,
    normal_hbm,
    rate_hbm,
    evolve_hbm,
    region_hbm,
    creep_hbm,
    v_out,
    d_out,
    s_out,
    step_out,
    kv,
    gathered,
    acc,
    xsend,
    xrecv,
    deficit,
    state,
    factor,
    step_in,
    load_in,
    normal_in,
    rate_in,
    evolve_in,
    region_in,
    creep_in,
    cols,
    top,
    mid,
    top_recv,
    mid_recv,
    k_sem,
    in_sem,
    send_sem,
    recv_sem,
    max_send,
    max_recv,
):
    members = deficit.shape[1]
    width = members // CHUNKS
    x = lax.axis_index("row_0")
    yl = lax.axis_index("row_1")
    yh = lax.axis_index("blk_0")
    z = lax.axis_index("blk_1")
    core = lax.axis_index("blk_2")

    z_up = {"blk_1": lax.rem(z + 1, 8)}
    z_down = {"blk_1": lax.rem(z + 7, 8)}
    y_far = {"blk_0": 1 - yh}
    sibling = {"blk_2": 1 - core}
    plane_peers = [
        {"row_0": lax.rem(x + dx, 4), "row_1": (yl + dl) % 2, "blk_0": (yh + dh) % 2}
        for dx in range(4)
        for dl in range(2)
        for dh in range(2)
        if dx or dl or dh
    ]
    line_peers = [
        {"blk_1": lax.rem(z + dz, 8), "blk_2": (core + dc) % 2}
        for dz in range(8)
        for dc in range(2)
        if dz or dc
    ]

    loads = []
    for i, (src, dst) in enumerate(
        (
            (deficit_hbm, deficit),
            (step_hbm, step_in),
            (load_hbm, load_in),
            (normal_hbm, normal_in),
            (rate_hbm, rate_in),
            (evolve_hbm, evolve_in),
            (region_hbm, region_in),
            (creep_hbm, creep_in),
            (state_hbm, state),
        )
    ):
        copy = pltpu.make_async_copy(src, dst, in_sem.at[i])
        copy.start()
        loads.append(copy)

    barrier = pltpu.get_barrier_semaphore()
    first_peers = [z_up, z_down, y_far, sibling] + [
        {"row_0": lax.rem(x + dx, 4), "row_1": (yl + dl) % 2} for dx, dl in ROW_OFFSETS
    ]
    for peer in first_peers:
        pl.semaphore_signal(barrier, inc=1, device_id=peer, device_id_type=MESH)

    for group, (low, high) in enumerate(GROUPS):
        for offset, plane, cr in itertools.product(OFFSETS[group], range(2), range(2)):
            at = slot(plane, offset, cr)
            block = (((yh + plane) % 2) * 8 + lax.rem(z + offset, 8)) * 2 + (core + cr) % 2
            pltpu.make_async_copy(
                k_hbm.at[:, pl.ds(pl.multiple_of(block * E, E), E)],
                kv.at[:, pl.ds(at * E, E)],
                k_sem.at[group],
            ).start()

    sent = []
    flight = {}

    def send(phase, key, src, dst, number, device):
        copy = pltpu.make_async_remote_copy(
            src_ref=src,
            dst_ref=dst,
            send_sem=send_sem.at[phase, number],
            recv_sem=recv_sem.at[phase, number],
            device_id=device,
            device_id_type=MESH,
        )
        copy.start()
        sent.append(copy)
        flight[(phase, key)] = copy

    def arrived(phase, *keys):
        for key in keys:
            flight[(phase, key)].wait_recv()

    def rows_of(phase, at, half=None):
        if half is None:
            return gathered.at[phase, pl.ds(at * E, E)]
        return gathered.at[phase, pl.ds(at * E + half * (E // 2), E // 2)]

    numbers = {}

    def number_of(key):
        return numbers.setdefault(key, len(numbers))

    def move(phase, plane, offset, to_plane, to_offset, device, half=None):
        key = (to_plane, to_offset, half)
        send(
            phase,
            key,
            rows_of(phase, slot(plane, offset, 0), half),
            rows_of(phase, slot(to_plane, to_offset, 0), half),
            number_of(key),
            device,
        )

    def share(phase, plane, *offsets):
        key = ("core", plane, offsets)
        at, to, count = slot(plane, offsets[0], 0), slot(plane, offsets[0], 1), len(offsets) * E
        send(
            phase,
            key,
            gathered.at[phase, pl.ds(at * E, count)],
            gathered.at[phase, pl.ds(to * E, count)],
            number_of(key),
            sibling,
        )

    def shared(phase, *parts):
        for offsets in parts:
            arrived(phase, ("core", 0, offsets), ("core", 1, offsets))

    def round_0(phase):
        move(phase, 0, 0, 0, 7, z_up)
        move(phase, 0, 0, 0, 1, z_down)
        move(phase, 0, 0, 1, 0, y_far)
        share(phase, 0, 0)

    def round_1(phase):
        arrived(phase, (0, 7, None))
        move(phase, 0, 7, 0, 6, z_up)
        move(phase, 0, 7, 1, 7, y_far, 1)
        arrived(phase, (0, 1, None))
        move(phase, 0, 1, 0, 2, z_down)
        move(phase, 0, 1, 1, 1, y_far, 1)
        arrived(phase, (1, 0, None))
        move(phase, 1, 0, 1, 7, z_up, 0)
        move(phase, 1, 0, 1, 1, z_down, 0)
        share(phase, 0, 7, 1)
        share(phase, 1, 0)

    def round_2(phase):
        arrived(phase, (0, 6, None))
        move(phase, 0, 6, 0, 5, z_up)
        move(phase, 0, 6, 1, 6, y_far, 1)
        arrived(phase, (0, 2, None))
        move(phase, 0, 2, 0, 3, z_down)
        move(phase, 0, 2, 1, 2, y_far, 1)
        arrived(phase, (1, 7, 0))
        move(phase, 1, 7, 1, 6, z_up, 0)
        arrived(phase, (1, 1, 0))
        move(phase, 1, 1, 1, 2, z_down, 0)
        share(phase, 0, 6, 2)
        arrived(phase, (1, 7, 1), (1, 1, 1))
        share(phase, 1, 7, 1)

    def round_3(phase):
        arrived(phase, (0, 5, None))
        move(phase, 0, 5, 0, 4, z_up, 0)
        move(phase, 0, 5, 1, 5, y_far, 1)
        arrived(phase, (0, 3, None))
        move(phase, 0, 3, 0, 4, z_down, 1)
        move(phase, 0, 3, 1, 3, y_far, 1)
        arrived(phase, (1, 6, 0))
        move(phase, 1, 6, 1, 5, z_up, 0)
        arrived(phase, (1, 2, 0))
        move(phase, 1, 2, 1, 3, z_down, 0)
        share(phase, 0, 5, 3)
        arrived(phase, (1, 6, 1), (1, 2, 1))
        share(phase, 1, 6, 2)

    def round_4(phase):
        arrived(phase, (0, 4, 1))
        move(phase, 0, 4, 1, 4, y_far, 1)
        arrived(phase, (1, 5, 0))
        move(phase, 1, 5, 1, 4, z_up, 0)
        arrived(phase, (0, 4, 0))
        share(phase, 0, 4)
        arrived(phase, (1, 3, 0), (1, 3, 1), (1, 5, 1))
        share(phase, 1, 5, 3)

    def round_5(phase):
        arrived(phase, (1, 4, 0), (1, 4, 1))
        share(phase, 1, 4)

    def product(phase, group):
        low, high = GROUPS[group]
        return jnp.dot(
            kv[:, low * E : high * E],
            gathered[phase, low * E : high * E, :],
            preferred_element_type=jnp.float32,
        )

    def multiply(phase, chunk, group):
        if phase == 0:
            low, high = GROUPS[group]
            part = kv.at[:, pl.ds(low * E, (high - low) * E)]
            pltpu.make_async_copy(part, part, k_sem.at[group]).wait()

        value = product(phase, group)
        if group == 0:
            acc[chunk] = value
        else:
            acc[chunk] += value

    def multiply_last(phase, chunk):
        multiply(phase, chunk, len(GROUPS) - 1)
        for k, (dx, dl) in enumerate(ROW_OFFSETS):
            base = (lax.rem(x + dx, 4) * 2 + (yl + dl) % 2) * E

            def tile(i, carry):
                rows = pl.ds(pl.multiple_of(base + i * 64, 64), 64)
                xsend[phase, k, pl.ds(pl.multiple_of(i * 64, 64), 64)] = acc[chunk, rows].astype(jnp.bfloat16)
                return carry

            lax.fori_loop(0, 2, tile, 0)
            send(
                phase,
                ("row", k),
                xsend.at[phase, k],
                xrecv.at[phase, k],
                number_of(("row", k)),
                {"row_0": lax.rem(x + dx, 4), "row_1": (yl + dl) % 2},
            )

    def set_factor(chunk):
        lanes = slice(chunk * width, (chunk + 1) * width)

        def tile(i, carry):
            rows = pl.ds(pl.multiple_of(i * 32, 32), 32)
            rate = cols[rows, 2:3]
            evolve = cols[rows, 3:4]
            factor[chunk, rows] = 0.5 * jnp.exp(evolve * jnp.log(state[rows, lanes]) / rate)
            return carry

        lax.fori_loop(0, 4, tile, 0)

    def solve(phase, chunk, step):
        lanes = slice(chunk * width, (chunk + 1) * width)
        arrived(phase, *(("row", k) for k in range(7)))
        own = (x * 2 + yl) * E
        step_now = step_in[:, lanes]

        def tile(i, carry):
            rows = pl.ds(pl.multiple_of(i * TILE, TILE), TILE)
            loading = cols[rows, 0:1]
            strength = cols[rows, 1:2] * cols[rows, 2:3]
            creeping = cols[rows, 4:5]
            total = acc[chunk, pl.ds(pl.multiple_of(own + i * TILE, TILE), TILE)]
            for k in range(7):
                total = total + xrecv[phase, k, rows].astype(jnp.float32)
            stress = loading + total
            scale = factor[chunk, rows]
            slope = strength * scale
            speed = stress / (slope + DAMPING)
            for _ in range(NEWTON):
                scaled = scale * speed
                magnitude = jnp.abs(scaled)
                root = jnp.sqrt(magnitude * magnitude + 1.0)
                arc = jnp.log(magnitude + root)
                arc = jnp.where(scaled < 0.0, -arc, arc)
                mismatch = strength * arc + DAMPING * speed - stress
                gradient = slope / root + DAMPING
                speed = speed - mismatch / gradient
            speed = jnp.where(creeping > 0.5, jnp.float32(PLATE_RATE), speed)
            size = jnp.abs(speed)
            if step == 0:
                old = state[rows, lanes]
                state[rows, lanes] = old * jnp.exp(step_now * (1.0 / old - size))
                moved = deficit[rows, lanes] + step_now * (speed - PLATE_RATE)
                deficit[rows, lanes] = moved
                gathered[phase + CHUNKS, pl.ds(pl.multiple_of(i * TILE, TILE), TILE)] = moved.astype(jnp.bfloat16)
            else:
                v_out[rows, lanes] = speed
            return jnp.maximum(carry, jnp.max(size.reshape(TILE // 8, 8, width), axis=0))

        largest = lax.fori_loop(0, E // TILE, tile, jnp.zeros((8, width), jnp.float32))
        top[step, :, lanes] = jnp.max(largest, axis=0, keepdims=True)

    max_copies = {}

    def max_send_all(step, stage):
        peers = plane_peers if stage == 0 else line_peers
        source = top if stage == 0 else mid
        target = top_recv if stage == 0 else mid_recv
        copies = []
        for k, peer in enumerate(peers):
            copy = pltpu.make_async_remote_copy(
                src_ref=source.at[step],
                dst_ref=target.at[step, k],
                send_sem=max_send.at[step, stage, k],
                recv_sem=max_recv.at[step, stage, k],
                device_id=peer,
                device_id_type=MESH,
            )
            copy.start()
            copies.append(copy)
            sent.append(copy)
        max_copies[(step, stage)] = copies

    def max_take(step, stage):
        for copy in max_copies[(step, stage)]:
            copy.wait_recv()
        source = top if stage == 0 else mid
        target = top_recv if stage == 0 else mid_recv
        return jnp.maximum(source[step], jnp.max(target[step], axis=0))

    outs = []
    loads[0].wait()
    for chunk in range(CHUNKS):
        gathered[chunk, 0:E] = deficit[:, chunk * width : (chunk + 1) * width].astype(jnp.bfloat16)
    for copy in loads[1:]:
        copy.wait()
    region = region_in[...]
    rate_row = jnp.zeros((1, E), jnp.float32)
    evolve_row = jnp.zeros((1, E), jnp.float32)
    for level in range(rate_in.shape[1]):
        chosen = region == level
        rate_row = jnp.where(chosen, rate_in[:, level : level + 1], rate_row)
        evolve_row = jnp.where(chosen, evolve_in[:, level : level + 1], evolve_row)
    creep_row = jnp.where(creep_in[...] == 1, 1.0, 0.0).astype(jnp.float32)
    picked = lax.broadcasted_iota(jnp.int32, (E, E), 0)
    stacked = jnp.zeros((E, E), jnp.float32)
    for k, row in enumerate((load_in[...], normal_in[...], rate_row, evolve_row, creep_row)):
        stacked = jnp.where(picked == k, jnp.broadcast_to(row, (E, E)), stacked)
    cols[...] = stacked.T

    pl.semaphore_wait(barrier, len(first_peers))

    first = list(range(CHUNKS))
    for chunk in first:
        round_0(chunk)
    for chunk in first:
        set_factor(chunk)

    for step in range(2):
        phases = [step * CHUNKS + chunk for chunk in range(CHUNKS)]
        def stage(k, chunk):
            phase = phases[chunk]
            if k == 1:
                round_1(phase)
            elif k == 2:
                round_2(phase)
                shared(phase, (0,))
                multiply(phase, chunk, 0)
            elif k == 3:
                round_3(phase)
                shared(phase, (7, 1))
                multiply(phase, chunk, 1)
                if step == 1 and chunk == 0:
                    mid[0] = max_take(0, 0)
                    max_send_all(0, 1)
            elif k == 4:
                round_4(phase)
                shared(phase, (6, 2))
                multiply(phase, chunk, 2)
            elif k == 5:
                round_5(phase)
                shared(phase, (5, 3), (4,))
                multiply_last(phase, chunk)
            elif k == 6:
                solve(phase, chunk, step)
                if step == 0:
                    round_0(phase + CHUNKS)

        plan = sorted((k, chunk, k) for k in range(1, 7) for chunk in range(CHUNKS))
        for _, chunk, k in plan:
            stage(k, chunk)
        max_send_all(step, 0)
        if step == 0:
            for chunk in range(CHUNKS):
                set_factor(chunk)


    step_last = STEP_CAP / (1.0 + max_take(0, 1))

    def finish(i, carry):
        rows = pl.ds(pl.multiple_of(i * 16, 16), 16)
        speed = v_out[rows]
        old = state[rows]
        s_out[rows] = old * jnp.exp(step_last * (1.0 / old - jnp.abs(speed)))
        d_out[rows] = deficit[rows] + step_last * (speed - PLATE_RATE)
        return carry

    lax.fori_loop(0, 8, finish, 0)
    mid[1] = max_take(1, 0)
    max_send_all(1, 1)
    step_out[...] = STEP_CAP / (1.0 + max_take(1, 1))
    for copy in sent:
        copy.wait_send()


def body(
    elastic_kernel,
    slip_deficit,
    state_variable,
    step_size,
    load_stress,
    normal_stress,
    rate_table,
    evolve_table,
    patch_region,
    creep_flag,
):
    members = slip_deficit.shape[3]
    width = members // CHUNKS
    phases = 2 * CHUNKS
    regions = rate_table.shape[0]
    f32, bf16, i32 = jnp.float32, jnp.bfloat16, jnp.int32
    anywhere = pl.BlockSpec(memory_space=pl.ANY)
    whole = pltpu.VMEM((E, members), f32)
    scratch = [
        pltpu.VMEM((1024, 4096), bf16),
        pltpu.VMEM((phases, 4096, width), bf16),
        pltpu.VMEM((CHUNKS, 1024, width), f32),
        pltpu.VMEM((phases, 7, E, width), bf16),
        pltpu.VMEM((phases, 7, E, width), bf16),
        pltpu.VMEM((E, members), f32),
        pltpu.VMEM((E, members), f32),
        pltpu.VMEM((CHUNKS, E, width), f32),
        pltpu.VMEM((1, members), f32),
        pltpu.VMEM((1, E), f32),
        pltpu.VMEM((1, E), f32),
        pltpu.VMEM((1, regions), f32),
        pltpu.VMEM((1, regions), f32),
        pltpu.VMEM((1, E), i32),
        pltpu.VMEM((1, E), i32),
        pltpu.VMEM((E, E), f32),
        pltpu.VMEM((2, 1, members), f32),
        pltpu.VMEM((2, 1, members), f32),
        pltpu.VMEM((2, 15, 1, members), f32),
        pltpu.VMEM((2, 15, 1, members), f32),
        pltpu.SemaphoreType.DMA((len(GROUPS),)),
        pltpu.SemaphoreType.DMA((9,)),
        pltpu.SemaphoreType.DMA((phases, 48)),
        pltpu.SemaphoreType.DMA((phases, 48)),
        pltpu.SemaphoreType.DMA((2, 2, 15)),
        pltpu.SemaphoreType.DMA((2, 2, 15)),
    ]
    velocity, deficit, state, step_next = pl.pallas_call(
        kernel_body,
        out_shape=(whole, whole, whole, pltpu.VMEM((1, members), f32)),
        in_specs=[anywhere] * 10,
        out_specs=(pl.BlockSpec(memory_space=pltpu.VMEM),) * 4,
        scratch_shapes=scratch,
        compiler_params=pltpu.CompilerParams(
            collective_id=0, has_side_effects=True, vmem_limit_bytes=LIMIT * 1024 * 1024
        ),
        name="fault_steps",
    )(
        elastic_kernel.reshape(1024, 4096),
        slip_deficit.reshape(E, members),
        state_variable.reshape(E, members),
        step_size.reshape(1, members),
        load_stress.reshape(1, E),
        normal_stress.reshape(1, E),
        rate_table.reshape(1, regions),
        evolve_table.reshape(1, regions),
        patch_region.reshape(1, E),
        creep_flag.reshape(1, E),
    )
    shape = slip_deficit.shape
    return velocity.reshape(shape), deficit.reshape(shape), state.reshape(shape), step_next.reshape(members)


def solution(mesh):
    torus = Mesh(mesh.devices.reshape(4, 2, 2, 8, 2), AXES)
    in_specs = (
        P(BLK, None, ROW, None),
        P(BLK, ROW, None, None),
        P(BLK, ROW, None, None),
        P(),
        P(BLK, ROW, None),
        P(BLK, ROW, None),
        P(),
        P(),
        P(BLK, ROW, None),
        P(BLK, ROW, None),
    )
    out_specs = (P(BLK, ROW, None, None), P(BLK, ROW, None, None), P(BLK, ROW, None, None), P())
    return jax.shard_map(body, mesh=torus, in_specs=in_specs, out_specs=out_specs, check_vma=False)
```

```python
import functools
import itertools

import jax
import jax.numpy as jnp
from jax import lax
from jax.experimental import pallas as pl
from jax.experimental.pallas import tpu as pltpu
from jax.sharding import Mesh
from jax.sharding import PartitionSpec as P

NEWTON = 3
DAMPING = 0.5
PLATE_RATE = 1.0
STEP_CAP = 0.5

AXES = ("row_0", "row_1", "blk_0", "blk_1", "blk_2")
BLK = ("blk_0", "blk_1", "blk_2")
ROW = ("row_0", "row_1")
MESH = pl.DeviceIdType.MESH

CHUNKS = 2
E = 128
TILE = 64
ROW_OFFSETS = ((2, 1), (2, 0), (1, 1), (3, 1), (1, 0), (3, 0), (0, 1))
OFFSETS = ((0,), (7, 1), (6, 2), (5, 3, 4))
GROUPS = ((0, 4), (4, 12), (12, 20), (20, 32))


LIMIT = 62


def slot(plane, offset, core):
    group = next(g for g, offsets in enumerate(OFFSETS) if offset in offsets)
    offsets = OFFSETS[group]
    return GROUPS[group][0] + (core * 2 + plane) * len(offsets) + offsets.index(offset)


def kernel_body(
    k_hbm,
    deficit_hbm,
    state_hbm,
    step_hbm,
    load_hbm,
    normal_hbm,
    rate_hbm,
    evolve_hbm,
    region_hbm,
    creep_hbm,
    v_out,
    d_out,
    s_out,
    step_out,
    kv,
    gathered,
    acc,
    xsend,
    xrecv,
    deficit,
    state,
    factor,
    step_in,
    load_in,
    normal_in,
    rate_in,
    evolve_in,
    region_in,
    creep_in,
    cols,
    top,
    mid,
    top_recv,
    mid_recv,
    k_sem,
    in_sem,
    send_sem,
    recv_sem,
    max_send,
    max_recv,
):
    members = deficit.shape[1]
    width = members // CHUNKS
    x = lax.axis_index("row_0")
    yl = lax.axis_index("row_1")
    yh = lax.axis_index("blk_0")
    z = lax.axis_index("blk_1")
    core = lax.axis_index("blk_2")

    z_up = {"blk_1": lax.rem(z + 1, 8)}
    z_down = {"blk_1": lax.rem(z + 7, 8)}
    y_far = {"blk_0": 1 - yh}
    sibling = {"blk_2": 1 - core}
    plane_peers = [
        {"row_0": lax.rem(x + dx, 4), "row_1": (yl + dl) % 2, "blk_0": (yh + dh) % 2}
        for dx in range(4)
        for dl in range(2)
        for dh in range(2)
        if dx or dl or dh
    ]
    line_peers = [
        {"blk_1": lax.rem(z + dz, 8), "blk_2": (core + dc) % 2}
        for dz in range(8)
        for dc in range(2)
        if dz or dc
    ]

    loads = []
    for i, (src, dst) in enumerate(
        (
            (deficit_hbm, deficit),
            (step_hbm, step_in),
            (load_hbm, load_in),
            (normal_hbm, normal_in),
            (rate_hbm, rate_in),
            (evolve_hbm, evolve_in),
            (region_hbm, region_in),
            (creep_hbm, creep_in),
            (state_hbm, state),
        )
    ):
        copy = pltpu.make_async_copy(src, dst, in_sem.at[i])
        copy.start()
        loads.append(copy)

    barrier = pltpu.get_barrier_semaphore()
    first_peers = [z_up, z_down, y_far, sibling] + [
        {"row_0": lax.rem(x + dx, 4), "row_1": (yl + dl) % 2} for dx, dl in ROW_OFFSETS
    ]
    for peer in first_peers:
        pl.semaphore_signal(barrier, inc=1, device_id=peer, device_id_type=MESH)

    for group, (low, high) in enumerate(GROUPS):
        for offset, plane, cr in itertools.product(OFFSETS[group], range(2), range(2)):
            at = slot(plane, offset, cr)
            block = (((yh + plane) % 2) * 8 + lax.rem(z + offset, 8)) * 2 + (core + cr) % 2
            pltpu.make_async_copy(
                k_hbm.at[:, pl.ds(pl.multiple_of(block * E, E), E)],
                kv.at[:, pl.ds(at * E, E)],
                k_sem.at[group],
            ).start()

    sent = []
    flight = {}

    def send(phase, key, src, dst, number, device):
        copy = pltpu.make_async_remote_copy(
            src_ref=src,
            dst_ref=dst,
            send_sem=send_sem.at[phase, number],
            recv_sem=recv_sem.at[phase, number],
            device_id=device,
            device_id_type=MESH,
        )
        copy.start()
        sent.append(copy)
        flight[(phase, key)] = copy

    def arrived(phase, *keys):
        for key in keys:
            flight[(phase, key)].wait_recv()

    def rows_of(phase, at, half=None):
        if half is None:
            return gathered.at[phase, pl.ds(at * E, E)]
        return gathered.at[phase, pl.ds(at * E + half * (E // 2), E // 2)]

    numbers = {}

    def number_of(key):
        return numbers.setdefault(key, len(numbers))

    def move(phase, plane, offset, to_plane, to_offset, device, half=None):
        key = (to_plane, to_offset, half)
        send(
            phase,
            key,
            rows_of(phase, slot(plane, offset, 0), half),
            rows_of(phase, slot(to_plane, to_offset, 0), half),
            number_of(key),
            device,
        )

    def share(phase, plane, *offsets):
        key = ("core", plane, offsets)
        at, to, count = slot(plane, offsets[0], 0), slot(plane, offsets[0], 1), len(offsets) * E
        send(
            phase,
            key,
            gathered.at[phase, pl.ds(at * E, count)],
            gathered.at[phase, pl.ds(to * E, count)],
            number_of(key),
            sibling,
        )

    def shared(phase, *parts):
        for offsets in parts:
            arrived(phase, ("core", 0, offsets), ("core", 1, offsets))

    def round_0(phase):
        move(phase, 0, 0, 0, 7, z_up)
        move(phase, 0, 0, 0, 1, z_down)
        move(phase, 0, 0, 1, 0, y_far)
        share(phase, 0, 0)

    def round_1(phase):
        arrived(phase, (0, 7, None))
        move(phase, 0, 7, 0, 6, z_up)
        move(phase, 0, 7, 1, 7, y_far, 1)
        arrived(phase, (0, 1, None))
        move(phase, 0, 1, 0, 2, z_down)
        move(phase, 0, 1, 1, 1, y_far, 1)
        arrived(phase, (1, 0, None))
        move(phase, 1, 0, 1, 7, z_up, 0)
        move(phase, 1, 0, 1, 1, z_down, 0)
        share(phase, 0, 7, 1)
        share(phase, 1, 0)

    def round_2(phase):
        arrived(phase, (0, 6, None))
        move(phase, 0, 6, 0, 5, z_up)
        move(phase, 0, 6, 1, 6, y_far, 1)
        arrived(phase, (0, 2, None))
        move(phase, 0, 2, 0, 3, z_down)
        move(phase, 0, 2, 1, 2, y_far, 1)
        arrived(phase, (1, 7, 0))
        move(phase, 1, 7, 1, 6, z_up, 0)
        arrived(phase, (1, 1, 0))
        move(phase, 1, 1, 1, 2, z_down, 0)
        share(phase, 0, 6, 2)
        arrived(phase, (1, 7, 1), (1, 1, 1))
        share(phase, 1, 7, 1)

    def round_3(phase):
        arrived(phase, (0, 5, None))
        move(phase, 0, 5, 0, 4, z_up, 0)
        move(phase, 0, 5, 1, 5, y_far, 1)
        arrived(phase, (0, 3, None))
        move(phase, 0, 3, 0, 4, z_down, 1)
        move(phase, 0, 3, 1, 3, y_far, 1)
        arrived(phase, (1, 6, 0))
        move(phase, 1, 6, 1, 5, z_up, 0)
        arrived(phase, (1, 2, 0))
        move(phase, 1, 2, 1, 3, z_down, 0)
        share(phase, 0, 5, 3)
        arrived(phase, (1, 6, 1), (1, 2, 1))
        share(phase, 1, 6, 2)

    def round_4(phase):
        arrived(phase, (0, 4, 1))
        move(phase, 0, 4, 1, 4, y_far, 1)
        arrived(phase, (1, 5, 0))
        move(phase, 1, 5, 1, 4, z_up, 0)
        arrived(phase, (0, 4, 0))
        share(phase, 0, 4)
        arrived(phase, (1, 3, 0), (1, 3, 1), (1, 5, 1))
        share(phase, 1, 5, 3)

    def round_5(phase):
        arrived(phase, (1, 4, 0), (1, 4, 1))
        share(phase, 1, 4)

    def product(phase, group):
        low, high = GROUPS[group]
        return jnp.dot(
            kv[:, low * E : high * E],
            gathered[phase, low * E : high * E, :],
            preferred_element_type=jnp.float32,
        )

    def multiply(phase, chunk, group):
        if phase == 0:
            low, high = GROUPS[group]
            part = kv.at[:, pl.ds(low * E, (high - low) * E)]
            pltpu.make_async_copy(part, part, k_sem.at[group]).wait()

        value = product(phase, group)
        if group == 0:
            acc[chunk] = value
        else:
            acc[chunk] += value

    def multiply_last(phase, chunk):
        multiply(phase, chunk, len(GROUPS) - 1)
        for k, (dx, dl) in enumerate(ROW_OFFSETS):
            base = (lax.rem(x + dx, 4) * 2 + (yl + dl) % 2) * E

            def tile(i, carry):
                rows = pl.ds(pl.multiple_of(base + i * 64, 64), 64)
                xsend[phase, k, pl.ds(pl.multiple_of(i * 64, 64), 64)] = acc[chunk, rows].astype(jnp.bfloat16)
                return carry

            lax.fori_loop(0, 2, tile, 0)
            send(
                phase,
                ("row", k),
                xsend.at[phase, k],
                xrecv.at[phase, k],
                number_of(("row", k)),
                {"row_0": lax.rem(x + dx, 4), "row_1": (yl + dl) % 2},
            )

    def set_factor(chunk):
        lanes = slice(chunk * width, (chunk + 1) * width)

        def tile(i, carry):
            rows = pl.ds(pl.multiple_of(i * 32, 32), 32)
            rate = cols[rows, 2:3]
            evolve = cols[rows, 3:4]
            factor[chunk, rows] = 0.5 * jnp.exp(evolve * jnp.log(state[rows, lanes]) / rate)
            return carry

        lax.fori_loop(0, 4, tile, 0)

    def solve(phase, chunk, step):
        lanes = slice(chunk * width, (chunk + 1) * width)
        arrived(phase, *(("row", k) for k in range(7)))
        own = (x * 2 + yl) * E
        step_now = step_in[:, lanes]

        def tile(i, carry):
            rows = pl.ds(pl.multiple_of(i * TILE, TILE), TILE)
            loading = cols[rows, 0:1]
            strength = cols[rows, 1:2] * cols[rows, 2:3]
            creeping = cols[rows, 4:5]
            total = acc[chunk, pl.ds(pl.multiple_of(own + i * TILE, TILE), TILE)]
            for k in range(7):
                total = total + xrecv[phase, k, rows].astype(jnp.float32)
            stress = loading + total
            scale = factor[chunk, rows]
            slope = strength * scale
            speed = stress / (slope + DAMPING)
            for _ in range(NEWTON):
                scaled = scale * speed
                magnitude = jnp.abs(scaled)
                root = jnp.sqrt(magnitude * magnitude + 1.0)
                arc = jnp.log(magnitude + root)
                arc = jnp.where(scaled < 0.0, -arc, arc)
                mismatch = strength * arc + DAMPING * speed - stress
                speed = speed - mismatch * root / (slope + DAMPING * root)
            speed = jnp.where(creeping > 0.5, jnp.float32(PLATE_RATE), speed)
            size = jnp.abs(speed)
            if step == 0:
                old = state[rows, lanes]
                state[rows, lanes] = old * jnp.exp(step_now * (1.0 / old - size))
                moved = deficit[rows, lanes] + step_now * (speed - PLATE_RATE)
                deficit[rows, lanes] = moved
                gathered[phase + CHUNKS, pl.ds(pl.multiple_of(i * TILE, TILE), TILE)] = moved.astype(jnp.bfloat16)
            else:
                v_out[rows, lanes] = speed
            return jnp.maximum(carry, jnp.max(size.reshape(TILE // 8, 8, width), axis=0))

        largest = lax.fori_loop(0, E // TILE, tile, jnp.zeros((8, width), jnp.float32))
        top[step, :, lanes] = jnp.max(largest, axis=0, keepdims=True)

    max_copies = {}

    def max_send_all(step, stage):
        peers = plane_peers if stage == 0 else line_peers
        source = top if stage == 0 else mid
        target = top_recv if stage == 0 else mid_recv
        copies = []
        for k, peer in enumerate(peers):
            copy = pltpu.make_async_remote_copy(
                src_ref=source.at[step],
                dst_ref=target.at[step, k],
                send_sem=max_send.at[step, stage, k],
                recv_sem=max_recv.at[step, stage, k],
                device_id=peer,
                device_id_type=MESH,
            )
            copy.start()
            copies.append(copy)
            sent.append(copy)
        max_copies[(step, stage)] = copies

    def max_take(step, stage):
        for copy in max_copies[(step, stage)]:
            copy.wait_recv()
        source = top if stage == 0 else mid
        target = top_recv if stage == 0 else mid_recv
        return jnp.maximum(source[step], jnp.max(target[step], axis=0))

    outs = []
    loads[0].wait()
    for chunk in range(CHUNKS):
        gathered[chunk, 0:E] = deficit[:, chunk * width : (chunk + 1) * width].astype(jnp.bfloat16)
    for copy in loads[1:]:
        copy.wait()
    region = region_in[...]
    rate_row = jnp.zeros((1, E), jnp.float32)
    evolve_row = jnp.zeros((1, E), jnp.float32)
    for level in range(rate_in.shape[1]):
        chosen = region == level
        rate_row = jnp.where(chosen, rate_in[:, level : level + 1], rate_row)
        evolve_row = jnp.where(chosen, evolve_in[:, level : level + 1], evolve_row)
    creep_row = jnp.where(creep_in[...] == 1, 1.0, 0.0).astype(jnp.float32)
    picked = lax.broadcasted_iota(jnp.int32, (E, E), 0)
    stacked = jnp.zeros((E, E), jnp.float32)
    for k, row in enumerate((load_in[...], normal_in[...], rate_row, evolve_row, creep_row)):
        stacked = jnp.where(picked == k, jnp.broadcast_to(row, (E, E)), stacked)
    cols[...] = stacked.T

    pl.semaphore_wait(barrier, len(first_peers))

    first = list(range(CHUNKS))
    for chunk in first:
        round_0(chunk)
    for chunk in first:
        set_factor(chunk)

    for step in range(2):
        phases = [step * CHUNKS + chunk for chunk in range(CHUNKS)]
        def stage(k, chunk):
            phase = phases[chunk]
            if k == 1:
                round_1(phase)
            elif k == 2:
                round_2(phase)
                shared(phase, (0,))
                multiply(phase, chunk, 0)
            elif k == 3:
                round_3(phase)
                shared(phase, (7, 1))
                multiply(phase, chunk, 1)
                if step == 1 and chunk == 0:
                    mid[0] = max_take(0, 0)
                    max_send_all(0, 1)
            elif k == 4:
                round_4(phase)
                shared(phase, (6, 2))
                multiply(phase, chunk, 2)
            elif k == 5:
                round_5(phase)
                shared(phase, (5, 3), (4,))
                multiply_last(phase, chunk)
            elif k == 6:
                solve(phase, chunk, step)
                if step == 0:
                    round_0(phase + CHUNKS)

        plan = sorted((k, chunk, k) for k in range(1, 7) for chunk in range(CHUNKS))
        for _, chunk, k in plan:
            stage(k, chunk)
        max_send_all(step, 0)
        if step == 0:
            for chunk in range(CHUNKS):
                set_factor(chunk)


    step_last = STEP_CAP / (1.0 + max_take(0, 1))

    def finish(i, carry):
        rows = pl.ds(pl.multiple_of(i * 16, 16), 16)
        speed = v_out[rows]
        old = state[rows]
        s_out[rows] = old * jnp.exp(step_last * (1.0 / old - jnp.abs(speed)))
        d_out[rows] = deficit[rows] + step_last * (speed - PLATE_RATE)
        return carry

    lax.fori_loop(0, 8, finish, 0)
    mid[1] = max_take(1, 0)
    max_send_all(1, 1)
    step_out[...] = STEP_CAP / (1.0 + max_take(1, 1))
    for copy in sent:
        copy.wait_send()


def body(
    elastic_kernel,
    slip_deficit,
    state_variable,
    step_size,
    load_stress,
    normal_stress,
    rate_table,
    evolve_table,
    patch_region,
    creep_flag,
):
    members = slip_deficit.shape[3]
    width = members // CHUNKS
    phases = 2 * CHUNKS
    regions = rate_table.shape[0]
    f32, bf16, i32 = jnp.float32, jnp.bfloat16, jnp.int32
    anywhere = pl.BlockSpec(memory_space=pl.ANY)
    whole = pltpu.VMEM((E, members), f32)
    scratch = [
        pltpu.VMEM((1024, 4096), bf16),
        pltpu.VMEM((phases, 4096, width), bf16),
        pltpu.VMEM((CHUNKS, 1024, width), f32),
        pltpu.VMEM((phases, 7, E, width), bf16),
        pltpu.VMEM((phases, 7, E, width), bf16),
        pltpu.VMEM((E, members), f32),
        pltpu.VMEM((E, members), f32),
        pltpu.VMEM((CHUNKS, E, width), f32),
        pltpu.VMEM((1, members), f32),
        pltpu.VMEM((1, E), f32),
        pltpu.VMEM((1, E), f32),
        pltpu.VMEM((1, regions), f32),
        pltpu.VMEM((1, regions), f32),
        pltpu.VMEM((1, E), i32),
        pltpu.VMEM((1, E), i32),
        pltpu.VMEM((E, E), f32),
        pltpu.VMEM((2, 1, members), f32),
        pltpu.VMEM((2, 1, members), f32),
        pltpu.VMEM((2, 15, 1, members), f32),
        pltpu.VMEM((2, 15, 1, members), f32),
        pltpu.SemaphoreType.DMA((len(GROUPS),)),
        pltpu.SemaphoreType.DMA((9,)),
        pltpu.SemaphoreType.DMA((phases, 48)),
        pltpu.SemaphoreType.DMA((phases, 48)),
        pltpu.SemaphoreType.DMA((2, 2, 15)),
        pltpu.SemaphoreType.DMA((2, 2, 15)),
    ]
    velocity, deficit, state, step_next = pl.pallas_call(
        kernel_body,
        out_shape=(whole, whole, whole, pltpu.VMEM((1, members), f32)),
        in_specs=[anywhere] * 10,
        out_specs=(pl.BlockSpec(memory_space=pltpu.VMEM),) * 4,
        scratch_shapes=scratch,
        compiler_params=pltpu.CompilerParams(
            collective_id=0, has_side_effects=True, vmem_limit_bytes=LIMIT * 1024 * 1024
        ),
        name="fault_steps",
    )(
        elastic_kernel.reshape(1024, 4096),
        slip_deficit.reshape(E, members),
        state_variable.reshape(E, members),
        step_size.reshape(1, members),
        load_stress.reshape(1, E),
        normal_stress.reshape(1, E),
        rate_table.reshape(1, regions),
        evolve_table.reshape(1, regions),
        patch_region.reshape(1, E),
        creep_flag.reshape(1, E),
    )
    shape = slip_deficit.shape
    return velocity.reshape(shape), deficit.reshape(shape), state.reshape(shape), step_next.reshape(members)


def solution(mesh):
    torus = Mesh(mesh.devices.reshape(4, 2, 2, 8, 2), AXES)
    in_specs = (
        P(BLK, None, ROW, None),
        P(BLK, ROW, None, None),
        P(BLK, ROW, None, None),
        P(),
        P(BLK, ROW, None),
        P(BLK, ROW, None),
        P(),
        P(),
        P(BLK, ROW, None),
        P(BLK, ROW, None),
    )
    out_specs = (P(BLK, ROW, None, None), P(BLK, ROW, None, None), P(BLK, ROW, None, None), P())
    return jax.shard_map(body, mesh=torus, in_specs=in_specs, out_specs=out_specs, check_vma=False)
```
